32 devices in a mesh: seg: 4 (over y, core), vid: 4 (over z), tp: 2 (over x).
Axes of the slice: x: 2, y: 2, z: 4, core: 2. Of those that a mesh axis runs over, the one named last changes fastest.
Arguments:
- tokens: bfloat16 [4, 2048, 2048], P('vid', 'seg', 'tp'), may hold values from -400 to 400
- key_weight: bfloat16 [2048, 2048], P('vid', 'tp'), may hold values from -0.125 to 0.125
- query_weight: bfloat16 [2048, 2048], P('vid', 'tp'), may hold values from -0.125 to 0.125
- latent_queries: bfloat16 [128, 2048], P(None, 'tp'), may hold values from -400 to 400
- init_memory: float32 [4, 128, 2048], P('vid', None, 'tp'), may hold values from -6 to 6
- forget: float32 [4, 4, 2048], P('vid', 'seg', 'tp'), may hold values from 0 to 1
Outputs:
- mixed: bfloat16 [4, 2048, 2048], P('vid', 'seg', 'tp')
- memory: float32 [4, 512, 2048], P('vid', 'seg', 'tp')
The draws below stay inside these ranges and needn't reach their ends.
All inputs are finite; a program needn't handle non-finite values.
Results may differ from the reference program's by a relative error of at most 0.015.
The reference program's roundings to bfloat16 on the way count: a program that leaves them out, or rounds other values in their place, can miss the bound.
Values may be sent and summed in bfloat16 or wider, within the bound.
A program may use at most 64 MiB of HBM per device.

```python
import jax
import jax.numpy as jnp
from jax import lax

D = 2048
HEAD = 128
M = 128
TOK = 512
HEADS = 16
SEGMENT_COUNT = 4
VIDEO_COUNT = 4
FRAMES = 2048


def draw_tokens(key, part):
    base = jax.random.normal(jax.random.fold_in(key, 11), (VIDEO_COUNT, FRAMES, D), jnp.float32)
    return jnp.clip(base, -400.0, 400.0).astype(jnp.bfloat16)


def draw_latent_queries(key, part):
    base = jax.random.normal(jax.random.fold_in(key, 21), (M, D), jnp.float32)
    return jnp.clip(base, -400.0, 400.0).astype(jnp.bfloat16)


def draw_forget(key, part):
    slow = 0.1 ** (1.0 / SEGMENT_COUNT)
    low = 0.02
    level = jax.random.uniform(jax.random.fold_in(key, 31), (VIDEO_COUNT, 1, D), jnp.float32)
    rate = jnp.exp(jnp.log(low) + level * (jnp.log(slow) - jnp.log(low)))
    power = jax.random.uniform(jax.random.fold_in(key, 32), (VIDEO_COUNT, SEGMENT_COUNT, D), jnp.float32, 0.5, 1.0)
    retained_memory = rate ** power
    segment_group = jax.random.randint(jax.random.fold_in(key, 33), (VIDEO_COUNT, SEGMENT_COUNT, 1), 0, 6) == 0
    training_loss = jax.random.uniform(jax.random.fold_in(key, 34), (VIDEO_COUNT, SEGMENT_COUNT, 1), jnp.float32, 0.5, 0.8)
    return retained_memory * jnp.where(segment_group, training_loss, 1.0)


def steps_of(stream_key, shape, pieces, smallest, largest):
    gain = 1.0
    for axis_at, parts in pieces:
        heights = jax.random.uniform(jax.random.fold_in(jax.random.fold_in(stream_key, 6), axis_at), (parts,), jnp.float32, smallest / len(pieces), largest / len(pieces))
        gain = gain * jnp.repeat(jnp.exp(heights), shape[axis_at] // parts).reshape((-1,) + (1,) * (len(shape) - 1 - axis_at))
    return gain


def bell_draw(key, shape, deviation, bound, split=(), held_as=jnp.bfloat16):
    result = deviation * jax.random.normal(key, shape, jnp.float32)
    if split:
        result = result * steps_of(key, shape, split, -0.22, 0.18)
    return jnp.clip(result, -bound, bound).astype(held_as)


def setup_inputs(seed: int = 0) -> dict:
    splits = jax.random.split(jax.random.key(seed), 7)
    tokens = draw_tokens(jax.random.fold_in(splits[6], 71), 0)
    key_weight = bell_draw(splits[1], (D, D), D ** -0.5, 0.125, ((0, 4), (1, 2)))
    query_weight = bell_draw(splits[2], (D, D), D ** -0.5, 0.125, ((0, 4), (1, 2)))
    latent_queries = draw_latent_queries(jax.random.fold_in(splits[6], 71), 0)
    init_memory = bell_draw(splits[4], (VIDEO_COUNT, M, D), 1.0, 6.0, ((0, 4), (2, 2)), jnp.float32)
    forget = draw_forget(jax.random.fold_in(splits[6], 71), 0)
    return dict(tokens=tokens, key_weight=key_weight, query_weight=query_weight, latent_queries=latent_queries, init_memory=init_memory, forget=forget)


def rounded(value):
    return lax.optimization_barrier(value.astype(jnp.bfloat16)).astype(jnp.float32)

def trailing_softmax(scores):
    top = lax.optimization_barrier(jnp.max(scores, axis=-1, keepdims=True))
    expo = jnp.exp(scores - top)
    return expo / lax.optimization_barrier(jnp.sum(expo, axis=-1, keepdims=True))

def resample(latent, keys, values):
    scores = jnp.einsum('mhe,the->hmt', latent, keys) / jnp.sqrt(jnp.float32(HEAD))
    weight_params = rounded(trailing_softmax(scores))
    return jnp.einsum('hmt,the->mhe', weight_params, values)

def readout(queries, memory_in):
    heads = memory_in.reshape(M, HEADS, HEAD)
    normed = heads * lax.rsqrt(lax.optimization_barrier(jnp.mean(heads * heads, axis=-1, keepdims=True)) + 1e-06)
    scores = jnp.einsum('the,mhe->htm', queries, rounded(normed)) / jnp.sqrt(jnp.float32(HEAD))
    weight_params = rounded(trailing_softmax(scores))
    return jnp.einsum('htm,mhe->the', weight_params, rounded(heads))

def reference(tokens, key_weight, query_weight, latent_queries, init_memory, forget):
    latent = latent_queries.astype(jnp.float32).reshape(M, HEADS, HEAD)

    def video(items):
        frames, initial_memory, retain = items
        keys = jnp.dot(frames, key_weight, preferred_element_type=jnp.float32).astype(jnp.bfloat16).astype(jnp.float32)
        queries = jnp.dot(frames, query_weight, preferred_element_type=jnp.float32).astype(jnp.bfloat16).astype(jnp.float32)
        keys = keys.reshape(SEGMENT_COUNT, TOK, HEADS, HEAD)
        queries = queries.reshape(SEGMENT_COUNT, TOK, HEADS, HEAD)
        values = frames.astype(jnp.float32).reshape(SEGMENT_COUNT, TOK, HEADS, HEAD)

        def step(memory_in, segment):
            seg_keys, seg_queries, seg_values, seg_retain = segment
            update = resample(latent, seg_keys, seg_values).reshape(M, D)
            read = readout(seg_queries, memory_in).reshape(TOK, D)
            mixed = (seg_values.reshape(TOK, D) + read).astype(jnp.bfloat16)
            memory_out = seg_retain[None, :] * memory_in + update
            return (memory_out, (mixed, memory_out))
        last, (mixed, memory) = lax.scan(step, initial_memory, (keys, queries, values, retain))
        return (mixed.reshape(FRAMES, D), memory.reshape(SEGMENT_COUNT * M, D))
    return lax.map(video, (tokens, init_memory, forget))
```

```python
import functools

import jax
import jax.numpy as jnp
from jax import lax
from jax.experimental import pallas as pl
from jax.experimental.pallas import tpu as pltpu
from jax.sharding import PartitionSpec as P

HEAD = 128


def from_behind(block, axis, distance):
    devices = range(lax.axis_size(axis))
    route = [(i - distance, i) for i in devices if i - distance in devices]
    return lax.ppermute(block, axis, route)


def trailing_softmax(scores):
    top = jnp.max(scores, axis=-1, keepdims=True)
    expo = jnp.exp(scores - top)
    return expo / jnp.sum(expo, axis=-1, keepdims=True)


def add_rows(left, piece):
    return jnp.dot(left, piece, preferred_element_type=jnp.float32)


def shards(tokens, key_weight, query_weight, latent_queries, init_memory, forget):
    local = tokens[0]
    width = local.shape[1]
    heads = width // HEAD
    latents = latent_queries.shape[0]
    whole = lax.all_gather(local, "tp", axis=1, tiled=True)

    def add_one(piece):
        return add_rows(whole, piece)

    keys_full = add_one(lax.all_gather(key_weight, "vid", axis=0, tiled=True))
    queries_full = add_one(lax.all_gather(query_weight, "vid", axis=0, tiled=True))
    scale = 1.0 / jnp.sqrt(jnp.float32(HEAD))
    keys = keys_full.astype(jnp.bfloat16).reshape(-1, heads, HEAD)
    queries = queries_full.astype(jnp.bfloat16).reshape(-1, heads, HEAD)
    values = local.reshape(-1, heads, HEAD)
    latent = latent_queries.reshape(latents, heads, HEAD)
    scores = jnp.einsum("mhe,the->hmt", latent, keys, preferred_element_type=jnp.float32) * scale
    weight_params = trailing_softmax(scores).astype(jnp.bfloat16)
    update = jnp.einsum(
        "hmt,the->mhe", weight_params, values, preferred_element_type=jnp.float32
    ).reshape(latents, width)
    retain = forget[0]
    initial_memory = init_memory[0]
    first = lax.axis_index("seg") == 0

    def turn(step, memory_now):
        received = from_behind(retain * memory_now + update, "seg", 1)
        return jnp.where(first, initial_memory, received)

    memory_in = lax.fori_loop(0, lax.axis_size("seg") - 1, turn, initial_memory)
    memory_out = retain * memory_in + update
    grouped = memory_in.reshape(latents, heads, HEAD)
    normed = grouped * lax.rsqrt(jnp.mean(grouped * grouped, axis=-1, keepdims=True) + 1e-06)
    read_scores = (
        jnp.einsum(
            "the,mhe->htm", queries, normed.astype(jnp.bfloat16), preferred_element_type=jnp.float32
        )
        * scale
    )
    read_weights = trailing_softmax(read_scores).astype(jnp.bfloat16)
    read = jnp.einsum(
        "htm,mhe->the",
        read_weights,
        grouped.astype(jnp.bfloat16),
        preferred_element_type=jnp.float32,
    )
    mixed = (local.astype(jnp.float32) + read.reshape(-1, width)).astype(jnp.bfloat16)
    return (mixed[None], memory_out[None])


CORES = 2


def softmax_rows(scores):
    top = jnp.max(scores, axis=-1, keepdims=True)
    expo = jnp.exp(scores - top)
    return (expo * (1.0 / jnp.sum(expo, axis=-1, keepdims=True))).astype(jnp.bfloat16)


def fused_kernel(
    segs, vids, tps,
    tokens, key_w, query_w, latent, init_memory, forget,
    mixed, memory_out,
    weights, tok, keys, queries, memory_in, update,
    load_sem, tok_send, tok_recv, z_send, z_recv, y_send, y_recv, d_send, d_recv, m_send, m_recv,
):
    chips = segs // CORES
    s, z, t = lax.axis_index("seg"), lax.axis_index("vid"), lax.axis_index("tp")
    y, core = s // CORES, s % CORES
    partner = y * CORES + (1 - core)
    width = tokens.shape[1]
    heads = width // HEAD
    rows = weights.shape[2] * weights.shape[3]
    sides = (1, -1)

    def remote(src, dst, send, recv, device):
        return pltpu.make_async_remote_copy(
            src_ref=src, dst_ref=dst, send_sem=send, recv_sem=recv,
            device_id=device, device_id_type=pl.DeviceIdType.MESH,
        )

    def z_copy(k, source, side):
        block = weights.at[k, source, s]
        return remote(block, block, z_send.at[k, source, (1 - side) // 2], z_recv.at[k, source], {"vid": z + side})

    def y_copy(k, source, chip, side):
        block = weights.at[k, source, chip * CORES + core]
        return remote(
            block, block, y_send.at[k, source, chip, (1 - side) // 2], y_recv.at[k, source, chip], {"seg": s + side * CORES}
        )

    def d_copy(k, source, chip, owner):
        block = weights.at[k, source, chip * CORES + owner]
        return remote(block, block, d_send.at[k, source, chip], d_recv.at[k, source, chip], {"seg": partner})

    def m_copy(h):
        cols = pl.ds(h * HEAD, HEAD)
        return remote(memory_out.at[:, cols], memory_in.at[:, cols], m_send.at[h], m_recv.at[h], {"seg": s + 1})

    def inside(index, size):
        return (index >= 0) & (index < size)

    def flag(condition):
        return jnp.where(condition, 1, 0).astype(jnp.int32)

    loads = [
        pltpu.make_async_copy(key_w, weights.at[0, z], load_sem.at[0]),
        pltpu.make_async_copy(tokens, tok.at[t], load_sem.at[1]),
        pltpu.make_async_copy(query_w, weights.at[1, z], load_sem.at[2]),
    ]
    for load in loads:
        load.start()
    first_memory = pltpu.make_async_copy(init_memory, memory_in, load_sem.at[3])

    @pl.when(s == 0)
    def _():
        first_memory.start()

    barrier = pltpu.get_barrier_semaphore()
    greeted = [
        (z + 1 < vids, {"vid": z + 1}),
        (z > 0, {"vid": z - 1}),
        (y + 1 < chips, {"seg": s + CORES}),
        (y > 0, {"seg": s - CORES}),
        ((core == 1) & (y + 1 < chips), {"seg": s + 1}),
        ((core == 0) & (y > 0), {"seg": s - 1}),
        (s >= 0, {"seg": partner}),
        (s >= 0, {"tp": 1 - t}),
    ]
    count = 0
    for condition, device in greeted:
        count = count + flag(condition)

        @pl.when(condition)
        def _(device=device):
            pl.semaphore_signal(barrier, inc=1, device_id=device, device_id_type=pl.DeviceIdType.MESH)

    pl.semaphore_wait(barrier, count)

    def own_sends(k):
        for side in sides:
            @pl.when(inside(z + side, vids))
            def _(side=side):
                z_copy(k, z, side).start()

    tok_copy = remote(tok.at[t], tok.at[t], tok_send, tok_recv, {"tp": 1 - t})
    loads[0].wait()
    own_sends(0)
    loads[1].wait()
    tok_copy.start()
    loads[2].wait()

    def each_source(distance, action):
        for side in sides:
            source = z - side * distance

            @pl.when(inside(source, vids))
            def _(source=source, side=side):
                action(source, side)

    def arrive_z(k, distance):
        def action(source, side):
            z_copy(k, source, side).wait_recv()

            @pl.when(inside(z + side, vids))
            def _():
                z_copy(k, source, side).start()

            for step in sides:
                @pl.when(inside(y + step, chips))
                def _(step=step):
                    y_copy(k, source, y, step).start()

            d_copy(k, source, y, core).start()

        each_source(distance, action)

    def each_chip(action):
        for gap in range(1, chips):
            for step in sides:
                chip = y - step * gap

                @pl.when(inside(chip, chips))
                def _(chip=chip, step=step):
                    action(chip, step)

    def arrive_y(k, distance):
        def action(source, side):
            def one(chip, step):
                y_copy(k, source, chip, step).wait_recv()

                @pl.when(inside(y + step, chips))
                def _():
                    y_copy(k, source, chip, step).start()

                d_copy(k, source, chip, core).start()

            each_chip(one)

        each_source(distance, action)

    def arrive_d(k, distance):
        def action(source, side):
            for chip in range(chips):
                d_copy(k, source, chip, 1 - core).wait_recv()

        each_source(distance, action)

    def project(k, out, begin, end):
        tile = 2 * HEAD
        for at in range(begin, end, tile):
            total = None
            for source in range(vids):
                left = tok[source * rows // width, :, pl.ds(source * rows % width, rows)]
                right = weights[k, source, :, :, pl.ds(at, tile)].reshape(rows, tile)
                term = jnp.dot(left, right, preferred_element_type=jnp.float32)
                total = term if total is None else total + term
            out[:, pl.ds(at, tile)] = total.astype(jnp.bfloat16)

    scale = 1.0 / jnp.sqrt(jnp.float32(HEAD))

    def resample(h):
        cols = pl.ds(h * HEAD, HEAD)
        scores = lax.dot_general(
            latent[:, cols], keys[:, cols], (((1,), (1,)), ((), ())), preferred_element_type=jnp.float32
        )
        update[:, cols] = jnp.dot(softmax_rows(scores * scale), tok[t, :, cols], preferred_element_type=jnp.float32)

    def carry(h):
        cols = pl.ds(h * HEAD, HEAD)

        @pl.when(s > 0)
        def _():
            remote(
                memory_out.at[:, cols], memory_in.at[:, cols], m_send.at[h], m_recv.at[h], {"seg": s - 1}
            ).wait_recv()

        memory_out[:, cols] = forget[:, cols] * memory_in[:, cols] + update[:, cols]

        @pl.when(s + 1 < segs)
        def _():
            m_copy(h).start()

    def readout(h):
        cols = pl.ds(h * HEAD, HEAD)
        held = memory_in[:, cols]
        normed = held * lax.rsqrt(jnp.mean(held * held, axis=-1, keepdims=True) + 1e-06)
        scores = lax.dot_general(
            queries[:, cols], normed.astype(jnp.bfloat16), (((1,), (1,)), ((), ())), preferred_element_type=jnp.float32
        )
        read = jnp.dot(softmax_rows(scores * scale), held.astype(jnp.bfloat16), preferred_element_type=jnp.float32)
        mixed[:, cols] = (tok[t, :, cols].astype(jnp.float32) + read).astype(jnp.bfloat16)

    events = sorted(
        [(distance, 0, distance) for distance in range(1, vids)]
        + [(distance + 1.5, 1, distance) for distance in range(1, vids)]
    )
    last_key = max(i for i, (_, k, _) in enumerate(events) if k == 0)
    for i, (_, k, distance) in enumerate(events[: last_key + 1]):
        arrive_z(k, distance)
        if i == 0:
            own_sends(1)
        else:
            arrive_y(*events[i - 1][1:])
    arrive_y(*events[last_key][1:])
    later = events[last_key + 1 :]
    arrive_z(*later[0][1:])
    for distance in range(1, vids):
        arrive_d(0, distance)
    tok_arrival = remote(tok.at[1 - t], tok.at[1 - t], tok_send, tok_recv, {"tp": 1 - t})
    tok_arrival.wait_recv()
    project(0, keys, 0, width)
    for i, event in enumerate(later[1:]):
        arrive_y(*later[i][1:])
        arrive_z(*event[1:])
    for h in range(heads):
        resample(h)

    @pl.when(s == 0)
    def _():
        first_memory.wait()

    for h in range(heads):
        carry(h)
    arrive_y(*later[-1][1:])
    for distance in range(1, vids):
        arrive_d(1, distance)
    project(1, queries, 0, width)
    for h in range(heads):
        readout(h)

    tok_copy.wait_send()
    for k in range(2):
        for side in sides:
            @pl.when(inside(z + side, vids))
            def _(k=k, side=side):
                z_copy(k, z, side).wait_send()

        for distance in range(1, vids):
            def sent(source, side, k=k):
                @pl.when(inside(z + side, vids))
                def _():
                    z_copy(k, source, side).wait_send()

                for step in sides:
                    @pl.when(inside(y + step, chips))
                    def _(step=step):
                        y_copy(k, source, y, step).wait_send()

                d_copy(k, source, y, core).wait_send()

                def one(chip, step):
                    @pl.when(inside(y + step, chips))
                    def _():
                        y_copy(k, source, chip, step).wait_send()

                    d_copy(k, source, chip, core).wait_send()

                each_chip(one)

            each_source(distance, sent)

    @pl.when(s + 1 < segs)
    def _():
        for h in range(heads):
            m_copy(h).wait_send()


def fused_shards(sizes, tokens, key_weight, query_weight, latent_queries, init_memory, forget):
    segs, vids, tps = sizes
    local = tokens[0]
    count, width = local.shape
    latents = latent_queries.shape[0]
    rows = key_weight.shape[0]
    heads = width // HEAD
    chips = segs // CORES
    parts = (segs, rows // segs, width)
    anywhere = pl.BlockSpec(memory_space=pl.ANY)
    vmem = pl.BlockSpec(memory_space=pltpu.VMEM)
    dma = pltpu.SemaphoreType.DMA
    mixed, memory = pl.pallas_call(
        functools.partial(fused_kernel, segs, vids, tps),
        out_shape=(
            jax.ShapeDtypeStruct((count, width), jnp.bfloat16),
            jax.ShapeDtypeStruct((latents, width), jnp.float32),
        ),
        in_specs=[anywhere, anywhere, anywhere, vmem, anywhere, vmem],
        out_specs=(vmem, vmem),
        scratch_shapes=[
            pltpu.VMEM((2, vids) + parts, jnp.bfloat16),
            pltpu.VMEM((tps, count, width), jnp.bfloat16),
            pltpu.VMEM((count, width), jnp.bfloat16),
            pltpu.VMEM((count, width), jnp.bfloat16),
            pltpu.VMEM((latents, width), jnp.float32),
            pltpu.VMEM((latents, width), jnp.float32),
            dma((4,)),
            dma,
            dma,
            dma((2, vids, 2)),
            dma((2, vids)),
            dma((2, vids, chips, 2)),
            dma((2, vids, chips)),
            dma((2, vids, chips)),
            dma((2, vids, chips)),
            dma((heads,)),
            dma((heads,)),
        ],
        compiler_params=pltpu.CompilerParams(collective_id=0, has_side_effects=True),
    )(
        local,
        key_weight.reshape(parts),
        query_weight.reshape(parts),
        latent_queries,
        init_memory[0],
        forget[0],
    )
    return (mixed[None], memory[None])


def relay_fits(segs, vids, tps):
    return tps == 2 and segs % CORES == 0 and vids > 2 and segs * vids <= 32


def solution(mesh):
    placed = (
        P("vid", "seg", "tp"),
        P("vid", "tp"),
        P("vid", "tp"),
        P(None, "tp"),
        P("vid", None, "tp"),
        P("vid", "seg", "tp"),
    )
    sizes = tuple(mesh.shape[axis] for axis in ("seg", "vid", "tp"))
    body = functools.partial(fused_shards, sizes) if relay_fits(*sizes) else shards
    return jax.shard_map(
        body,
        mesh=mesh,
        in_specs=placed,
        out_specs=(P("vid", "seg", "tp"), P("vid", "seg", "tp")),
        check_vma=False,
    )
```

```python
import functools

import jax
import jax.numpy as jnp
from jax import lax
from jax.experimental import pallas as pl
from jax.experimental.pallas import tpu as pltpu
from jax.sharding import PartitionSpec as P

HEAD = 128


def from_behind(block, axis, distance):
    devices = range(lax.axis_size(axis))
    route = [(i - distance, i) for i in devices if i - distance in devices]
    return lax.ppermute(block, axis, route)


def trailing_softmax(scores):
    top = jnp.max(scores, axis=-1, keepdims=True)
    expo = jnp.exp(scores - top)
    return expo / jnp.sum(expo, axis=-1, keepdims=True)


def add_rows(left, piece):
    return jnp.dot(left, piece, preferred_element_type=jnp.float32)


def shards(tokens, key_weight, query_weight, latent_queries, init_memory, forget):
    local = tokens[0]
    width = local.shape[1]
    heads = width // HEAD
    latents = latent_queries.shape[0]
    whole = lax.all_gather(local, "tp", axis=1, tiled=True)

    def add_one(piece):
        return add_rows(whole, piece)

    keys_full = add_one(lax.all_gather(key_weight, "vid", axis=0, tiled=True))
    queries_full = add_one(lax.all_gather(query_weight, "vid", axis=0, tiled=True))
    scale = 1.0 / jnp.sqrt(jnp.float32(HEAD))
    keys = keys_full.astype(jnp.bfloat16).reshape(-1, heads, HEAD)
    queries = queries_full.astype(jnp.bfloat16).reshape(-1, heads, HEAD)
    values = local.reshape(-1, heads, HEAD)
    latent = latent_queries.reshape(latents, heads, HEAD)
    scores = jnp.einsum("mhe,the->hmt", latent, keys, preferred_element_type=jnp.float32) * scale
    weight_params = trailing_softmax(scores).astype(jnp.bfloat16)
    update = jnp.einsum(
        "hmt,the->mhe", weight_params, values, preferred_element_type=jnp.float32
    ).reshape(latents, width)
    retain = forget[0]
    initial_memory = init_memory[0]
    first = lax.axis_index("seg") == 0

    def turn(step, memory_now):
        received = from_behind(retain * memory_now + update, "seg", 1)
        return jnp.where(first, initial_memory, received)

    memory_in = lax.fori_loop(0, lax.axis_size("seg") - 1, turn, initial_memory)
    memory_out = retain * memory_in + update
    grouped = memory_in.reshape(latents, heads, HEAD)
    normed = grouped * lax.rsqrt(jnp.mean(grouped * grouped, axis=-1, keepdims=True) + 1e-06)
    read_scores = (
        jnp.einsum(
            "the,mhe->htm", queries, normed.astype(jnp.bfloat16), preferred_element_type=jnp.float32
        )
        * scale
    )
    read_weights = trailing_softmax(read_scores).astype(jnp.bfloat16)
    read = jnp.einsum(
        "htm,mhe->the",
        read_weights,
        grouped.astype(jnp.bfloat16),
        preferred_element_type=jnp.float32,
    )
    mixed = (local.astype(jnp.float32) + read.reshape(-1, width)).astype(jnp.bfloat16)
    return (mixed[None], memory_out[None])


SPLITS = 2
CORES = 2


def softmax_rows(scores):
    top = jnp.max(scores, axis=-1, keepdims=True)
    expo = jnp.exp(scores - top)
    return (expo * (1.0 / jnp.sum(expo, axis=-1, keepdims=True))).astype(jnp.bfloat16)


def fused_kernel(
    segs, vids, tps,
    tokens, key_w, query_w, latent, init_memory, forget,
    mixed, memory_out,
    weights, tok, keys, queries, memory_in, update, partial,
    load_sem, tok_send, tok_recv, z_send, z_recv, y_send, y_recv, d_send, d_recv, m_send, m_recv,
):
    chips = segs // CORES
    s, z, t = lax.axis_index("seg"), lax.axis_index("vid"), lax.axis_index("tp")
    y, core = s // CORES, s % CORES
    partner = y * CORES + (1 - core)
    width = tokens.shape[1]
    heads = width // HEAD
    rows = weights.shape[2] * weights.shape[3]
    streams = range(2 * SPLITS)
    sides = (1, -1)

    def remote(src, dst, send, recv, device):
        return pltpu.make_async_remote_copy(
            src_ref=src, dst_ref=dst, send_sem=send, recv_sem=recv,
            device_id=device, device_id_type=pl.DeviceIdType.MESH,
        )

    def z_copy(k, source, side):
        block = weights.at[k, source, s]
        return remote(block, block, z_send.at[k, source, (1 - side) // 2], z_recv.at[k, source], {"vid": z + side})

    def y_copy(k, source, chip, side):
        block = weights.at[k, source, chip * CORES + core]
        return remote(
            block, block, y_send.at[k, source, chip, (1 - side) // 2], y_recv.at[k, source, chip], {"seg": s + side * CORES}
        )

    def d_copy(k, source, chip, owner):
        block = weights.at[k, source, chip * CORES + owner]
        return remote(block, block, d_send.at[k, source, chip], d_recv.at[k, source, chip], {"seg": partner})

    def m_copy(h):
        cols = pl.ds(h * HEAD, HEAD)
        return remote(memory_out.at[:, cols], memory_in.at[:, cols], m_send.at[h], m_recv.at[h], {"seg": s + 1})

    def inside(index, size):
        return (index >= 0) & (index < size)

    def flag(condition):
        return jnp.where(condition, 1, 0).astype(jnp.int32)

    tok_load = pltpu.make_async_copy(tokens, tok.at[t], load_sem.at[0])
    first_memory = pltpu.make_async_copy(init_memory, memory_in, load_sem.at[1])
    loads = [
        pltpu.make_async_copy((key_w, query_w)[k // SPLITS].at[k % SPLITS], weights.at[k, z], load_sem.at[2 + k])
        for k in streams
    ]
    key_streams, query_streams = streams[:SPLITS], streams[SPLITS:]
    for load in loads[:SPLITS] + [tok_load] + loads[SPLITS:]:
        load.start()

    @pl.when(s == 0)
    def _():
        first_memory.start()

    barrier = pltpu.get_barrier_semaphore()
    greeted = [
        (z + 1 < vids, {"vid": z + 1}),
        (z > 0, {"vid": z - 1}),
        (y + 1 < chips, {"seg": s + CORES}),
        (y > 0, {"seg": s - CORES}),
        ((core == 1) & (y + 1 < chips), {"seg": s + 1}),
        ((core == 0) & (y > 0), {"seg": s - 1}),
        (s >= 0, {"seg": partner}),
        (s >= 0, {"tp": 1 - t}),
    ]
    count = 0
    for condition, device in greeted:
        count = count + flag(condition)

        @pl.when(condition)
        def _(device=device):
            pl.semaphore_signal(barrier, inc=1, device_id=device, device_id_type=pl.DeviceIdType.MESH)

    pl.semaphore_wait(barrier, count)

    def own_sends(k):
        for side in sides:
            @pl.when(inside(z + side, vids))
            def _(side=side):
                z_copy(k, z, side).start()

    tok_copy = remote(tok.at[t], tok.at[t], tok_send, tok_recv, {"tp": 1 - t})
    for k in key_streams:
        loads[k].wait()
        own_sends(k)
    tok_load.wait()
    tok_copy.start()
    for k in query_streams:
        loads[k].wait()

    def each_source(distance, action):
        for side in sides:
            source = z - side * distance

            @pl.when(inside(source, vids))
            def _(source=source, side=side):
                action(source, side)

    def arrive_z(k, distance):
        def action(source, side):
            z_copy(k, source, side).wait_recv()

            @pl.when(inside(z + side, vids))
            def _():
                z_copy(k, source, side).start()

            for step in sides:
                @pl.when(inside(y + step, chips))
                def _(step=step):
                    y_copy(k, source, y, step).start()

            d_copy(k, source, y, core).start()

        each_source(distance, action)

    def each_chip(action):
        for gap in range(1, chips):
            for step in sides:
                chip = y - step * gap

                @pl.when(inside(chip, chips))
                def _(chip=chip, step=step):
                    action(chip, step)

    def arrive_y(k, distance):
        def action(source, side):
            def one(chip, step):
                y_copy(k, source, chip, step).wait_recv()

                @pl.when(inside(y + step, chips))
                def _():
                    y_copy(k, source, chip, step).start()

                d_copy(k, source, chip, core).start()

            each_chip(one)

        each_source(distance, action)

    last = jnp.where(2 * z < vids, vids - 1, 0)

    def arrive_d(k, distance, final=None):
        def action(source, side):
            def take():
                for chip in range(chips):
                    d_copy(k, source, chip, 1 - core).wait_recv()

            if final is None:
                take()
            else:
                pl.when((source == last) == final)(take)

        each_source(distance, action)

    tile = 2 * HEAD

    def product(first, sources, at):
        total = None
        for source in sources:
            begin = source * rows * SPLITS
            for part in range(SPLITS):
                place = pl.multiple_of(begin % width + part * rows, rows)
                left = tok[begin // width, :, pl.ds(place, rows)]
                right = weights[first + part, source, :, :, pl.ds(at, tile)].reshape(rows, tile)
                term = jnp.dot(left, right, preferred_element_type=jnp.float32)
                total = term if total is None else total + term
        return total

    scale = 1.0 / jnp.sqrt(jnp.float32(HEAD))

    def resample(h):
        cols = pl.ds(h * HEAD, HEAD)
        scores = lax.dot_general(
            latent[:, cols], keys[:, cols], (((1,), (1,)), ((), ())), preferred_element_type=jnp.float32
        )
        update[:, cols] = jnp.dot(softmax_rows(scores * scale), tok[t, :, cols], preferred_element_type=jnp.float32)

    def carry(h):
        cols = pl.ds(h * HEAD, HEAD)

        @pl.when(s > 0)
        def _():
            remote(
                memory_out.at[:, cols], memory_in.at[:, cols], m_send.at[h], m_recv.at[h], {"seg": s - 1}
            ).wait_recv()

        memory_out[:, cols] = forget[:, cols] * memory_in[:, cols] + update[:, cols]

        @pl.when(s + 1 < segs)
        def _():
            m_copy(h).start()

    def readout(h):
        cols = pl.ds(h * HEAD, HEAD)
        held = memory_in[:, cols]
        normed = held * lax.rsqrt(jnp.mean(held * held, axis=-1, keepdims=True) + 1e-06)
        scores = lax.dot_general(
            queries[:, cols], normed.astype(jnp.bfloat16), (((1,), (1,)), ((), ())), preferred_element_type=jnp.float32
        )
        read = jnp.dot(softmax_rows(scores * scale), held.astype(jnp.bfloat16), preferred_element_type=jnp.float32)
        mixed[:, cols] = (tok[t, :, cols].astype(jnp.float32) + read).astype(jnp.bfloat16)

    def arrive_all_z(group, distance):
        for k in group:
            arrive_z(k, distance)

    def arrive_all_y(group, distance):
        for k in group:
            arrive_y(k, distance)

    for distance in range(1, vids):
        arrive_all_z(key_streams, distance)
        if distance == vids - 2:
            for k in query_streams:
                own_sends(k)
        if distance > 1:
            arrive_all_y(key_streams, distance - 1)
    arrive_all_y(key_streams, vids - 1)
    arrive_all_z(query_streams, 1)
    for distance in range(1, vids):
        for k in key_streams:
            arrive_d(k, distance)
    remote(tok.at[1 - t], tok.at[1 - t], tok_send, tok_recv, {"tp": 1 - t}).wait_recv()
    for at in range(0, width, tile):
        keys[:, pl.ds(at, tile)] = product(0, range(vids), at).astype(jnp.bfloat16)
    arrive_all_y(query_streams, 1)
    for h in range(heads // 2):
        resample(h)
    for distance in range(2, vids - 1):
        arrive_all_z(query_streams, distance)
    for h in range(heads // 2, heads):
        resample(h)

    @pl.when(s == 0)
    def _():
        first_memory.wait()

    @pl.when(y == 0)
    def _():
        for h in range(heads):
            carry(h)

    for distance in range(2, vids - 1):
        arrive_all_y(query_streams, distance)
    arrive_all_z(query_streams, vids - 1)
    for distance in range(1, vids - 1):
        for k in query_streams:
            arrive_d(k, distance, final=False)
    others = [(last + 1 + i) % vids for i in range(vids - 1)]
    for at in range(0, width, tile):
        partial[:, pl.ds(at, tile)] = product(SPLITS, others, at)

    @pl.when(y > 0)
    def _():
        for h in range(heads):
            carry(h)

    arrive_all_y(query_streams, vids - 1)
    for distance in range(1, vids):
        for k in query_streams:
            arrive_d(k, distance, final=True)
    per_tile = tile // HEAD
    for at in range(0, width, tile):
        cols = pl.ds(at, tile)
        queries[:, cols] = (partial[:, cols] + product(SPLITS, [last], at)).astype(jnp.bfloat16)
        for h in range(at // HEAD, at // HEAD + per_tile):
            readout(h)

    tok_copy.wait_send()
    for k in streams:
        for side in sides:
            @pl.when(inside(z + side, vids))
            def _(k=k, side=side):
                z_copy(k, z, side).wait_send()

        for distance in range(1, vids):
            def sent(source, side, k=k):
                @pl.when(inside(z + side, vids))
                def _():
                    z_copy(k, source, side).wait_send()

                for step in sides:
                    @pl.when(inside(y + step, chips))
                    def _(step=step):
                        y_copy(k, source, y, step).wait_send()

                d_copy(k, source, y, core).wait_send()

                def one(chip, step):
                    @pl.when(inside(y + step, chips))
                    def _():
                        y_copy(k, source, chip, step).wait_send()

                    d_copy(k, source, chip, core).wait_send()

                each_chip(one)

            each_source(distance, sent)

    @pl.when(s + 1 < segs)
    def _():
        for h in range(heads):
            m_copy(h).wait_send()


def fused_shards(sizes, tokens, key_weight, query_weight, latent_queries, init_memory, forget):
    segs, vids, tps = sizes
    local = tokens[0]
    count, width = local.shape
    latents = latent_queries.shape[0]
    rows = key_weight.shape[0]
    heads = width // HEAD
    chips = segs // CORES
    parts = (segs, rows // segs // SPLITS, width)
    streams = 2 * SPLITS
    anywhere = pl.BlockSpec(memory_space=pl.ANY)
    vmem = pl.BlockSpec(memory_space=pltpu.VMEM)
    dma = pltpu.SemaphoreType.DMA
    mixed, memory = pl.pallas_call(
        functools.partial(fused_kernel, segs, vids, tps),
        out_shape=(
            jax.ShapeDtypeStruct((count, width), jnp.bfloat16),
            jax.ShapeDtypeStruct((latents, width), jnp.float32),
        ),
        in_specs=[anywhere, anywhere, anywhere, vmem, anywhere, vmem],
        out_specs=(vmem, vmem),
        scratch_shapes=[
            pltpu.VMEM((streams, vids) + parts, jnp.bfloat16),
            pltpu.VMEM((tps, count, width), jnp.bfloat16),
            pltpu.VMEM((count, width), jnp.bfloat16),
            pltpu.VMEM((count, width), jnp.bfloat16),
            pltpu.VMEM((latents, width), jnp.float32),
            pltpu.VMEM((latents, width), jnp.float32),
            pltpu.VMEM((count, width), jnp.float32),
            dma((2 + streams,)),
            dma,
            dma,
            dma((streams, vids, 2)),
            dma((streams, vids)),
            dma((streams, vids, chips, 2)),
            dma((streams, vids, chips)),
            dma((streams, vids, chips)),
            dma((streams, vids, chips)),
            dma((heads,)),
            dma((heads,)),
        ],
        compiler_params=pltpu.CompilerParams(collective_id=0, has_side_effects=True),
    )(
        local,
        key_weight.reshape((SPLITS,) + parts),
        query_weight.reshape((SPLITS,) + parts),
        latent_queries,
        init_memory[0],
        forget[0],
    )
    return (mixed[None], memory[None])


def relay_fits(segs, vids, tps):
    return tps == 2 and segs % CORES == 0 and vids > 2 and segs * vids <= 32


def solution(mesh):
    placed = (
        P("vid", "seg", "tp"),
        P("vid", "tp"),
        P("vid", "tp"),
        P(None, "tp"),
        P("vid", None, "tp"),
        P("vid", "seg", "tp"),
    )
    sizes = tuple(mesh.shape[axis] for axis in ("seg", "vid", "tp"))
    body = functools.partial(fused_shards, sizes) if relay_fits(*sizes) else shards
    return jax.shard_map(
        body,
        mesh=mesh,
        in_specs=placed,
        out_specs=(P("vid", "seg", "tp"), P("vid", "seg", "tp")),
        check_vma=False,
    )
```
